32 devices in a mesh: ta: 4 (over x, core), tb: 8 (over z, y).
Axes of the slice: x: 2, y: 2, z: 4, core: 2. Of those that a mesh axis runs over, the one named last changes fastest.
Arguments:
- theta_cube: bfloat16 [32, 90, 4096], P(('ta', 'tb')), may hold values from -20 to 20, as said below
- station_permutation_map: int32 [128], replicated, may hold values from 0 to 127, each once
- station_bathymetry_group: int32 [4096], replicated, may hold values from 0 to 15
- baroclinic_basis: bfloat16 [16, 90, 90], replicated, may hold values from -0.625 to 0.625
Outputs:
- anomaly_coef: bfloat16 [90, 32, 4096], P(None, None, ('ta', 'tb'))
The draws below stay inside these ranges and needn't reach their ends.
Inputs may be any that keep to these rules, and one draw needn't show every extreme that they name: `theta_cube`: temperature is a level-and-column profile plus time variation.
All inputs are finite; a program needn't handle non-finite values.
Results may differ from the reference program's by a relative error of at most 0.001.
Values may be sent and summed in bfloat16 or wider, within the bound.
A program may use at most 128 MiB of HBM per device.

```python
import jax
import jax.numpy as jnp
from jax import lax

LEV = 90
MODES = 90
CLASSES = 16
TILE = 32
PROBES_PER_CHIP = 128
SNAPS = 32
COLS = 4096
GROUPS = 128


def draw_theta_cube(key, part):
    first, second = jax.random.split(key, 2)
    profile = jax.random.uniform(first, (1, LEV, COLS), minval=-4.0, maxval=4.0)
    noise = jnp.clip(jax.random.normal(second, (SNAPS, LEV, COLS)), -6.0, 6.0)
    return (profile + noise).astype(jnp.bfloat16)


def set_ends(array, key, low, top_value):
    place = [jax.random.randint(jax.random.fold_in(key, axis), (), 0, length) for axis, length in enumerate(array.shape)]
    widest = array.shape.index(max(array.shape))
    neighbour = place[:widest] + [(place[widest] + 1) % array.shape[widest]] + place[widest + 1:]
    return array.at[tuple(place)].set(low).at[tuple(neighbour)].set(top_value)


def scatter_about(key, extent, spread, bound, kind=jnp.bfloat16):
    values = spread * jax.random.normal(key, extent, jnp.float32)
    return jnp.clip(values, min=-bound, max=bound).astype(kind)


def setup_inputs(seed: int = 0) -> dict:
    arg_keys = jax.random.split(jax.random.key(seed), 5)
    return {
        "theta_cube": draw_theta_cube(jax.random.fold_in(arg_keys[4], 71), 0),
        "station_permutation_map": jax.random.permutation(arg_keys[1], GROUPS).astype(jnp.int32),
        "station_bathymetry_group": set_ends(jax.random.randint(arg_keys[2], (COLS,), 0, CLASSES), jax.random.fold_in(arg_keys[2], 1), 0, CLASSES - 1).astype(jnp.int32),
        "baroclinic_basis": scatter_about(arg_keys[3], (CLASSES, LEV, MODES), LEV ** -0.5, 0.625),
    }


def reference(theta_cube, station_permutation_map, station_bathymetry_group, baroclinic_basis):
    offsets = jnp.arange(TILE, dtype=jnp.int32)
    source = (station_permutation_map.astype(jnp.int32)[:, None] * TILE + offsets[None, :]).reshape(-1)

    def one_block(probe_ordinal):
        probe_thermal_readings = jnp.take(theta_cube, probe_ordinal, axis=2).astype(jnp.float32)
        selected_probes = jnp.take(baroclinic_basis, jnp.take(station_bathymetry_group, probe_ordinal, axis=0), axis=0).astype(jnp.float32)
        modal_amplitude = jnp.einsum('btq,qtf->fbq', probe_thermal_readings, selected_probes)
        mean_coef = jnp.mean(modal_amplitude, axis=1, keepdims=True)
        return (modal_amplitude - mean_coef).astype(jnp.bfloat16)

    blocks = lax.map(one_block, source.reshape(-1, PROBES_PER_CHIP).astype(jnp.int32))
    return jnp.transpose(blocks, (1, 2, 0, 3)).reshape(MODES, SNAPS, COLS)
```

```python
import functools

import jax
import jax.numpy as jnp
from jax import lax
from jax.experimental import pallas as pl
from jax.experimental.pallas import tpu as pltpu
from jax.sharding import PartitionSpec as P

TILE = 32
MESH = pl.DeviceIdType.MESH
ROWS = 16


def exchange_kernel(
    n_ta, n_tb, col_dev,
    perm_ref, theta_ref, cls_ref, basis_ref,
    coef_ref, total_ref,
    turned_theta, turned_cls, send_buf, recv_buf, basis_rows, basis_t, mask, send_sem, recv_sem,
):
    n = n_ta * n_tb
    ta, tb = lax.axis_index("ta"), lax.axis_index("tb")
    me = ta * n_tb + tb
    _, lev, _ = theta_ref.shape
    classes, _, modes = basis_ref.shape
    pad = recv_buf.shape[1]
    per = col_dev // TILE

    barrier = pltpu.get_barrier_semaphore()

    def greet(k, _):
        other = lax.rem(me + k, n)
        pl.semaphore_signal(
            barrier, inc=1, device_id=(lax.div(other, n_tb), lax.rem(other, n_tb)), device_id_type=MESH
        )
        return 0

    lax.fori_loop(1, n, greet, 0)

    lane_group = lax.broadcasted_iota(jnp.int32, (1, col_dev), 1) // TILE

    def turn(block, _):
        lanes = pl.ds(pl.multiple_of(block * col_dev, col_dev), col_dev)
        piece = theta_ref[0, :, lanes].astype(jnp.float32)
        for k in range(per):
            turned_theta[k, block] = (pltpu.roll(piece, k * TILE, 1) if k else piece).astype(jnp.bfloat16)
        return 0

    lax.fori_loop(0, n, turn, 0)
    for k in range(per):
        turned_cls[k] = pltpu.roll(cls_ref[...], k * TILE, 1) if k else cls_ref[...]

    def regroup(dest, load):
        out = None
        for k in range(per):
            g = perm_ref[dest * per + k]
            shift = lax.rem(k + per - lax.rem(g, per), per)
            piece = load(shift, lax.div(g, per))
            out = piece if out is None else jnp.where(lane_group == k, piece, out)
        return out

    def prepare(dest, _):
        send_buf[dest] = regroup(dest, lambda shift, block: turned_theta[shift, block])
        return 0

    lax.fori_loop(0, n, prepare, 0)
    recv_buf[:, lev:, :] = jnp.zeros((n, pad - lev, col_dev), jnp.bfloat16)
    recv_buf[me, :lev, :] = send_buf[me]

    pl.semaphore_wait(barrier, n - 1)

    def offset(i):
        half = lax.div(i + 1, 2)
        odd = lax.rem(i, 2)
        return lax.rem(n_tb // 2 + odd * half + (1 - odd) * (n_tb - half), n_tb)

    def copy(src, dst, device):
        return pltpu.make_async_remote_copy(
            src_ref=send_buf.at[src],
            dst_ref=recv_buf.at[dst, pl.ds(0, lev), :],
            send_sem=send_sem.at[src],
            recv_sem=recv_sem.at[dst],
            device_id=device,
            device_id_type=MESH,
        )

    def send(i, a):
        to_ta, to_tb = lax.rem(ta + a, n_ta), lax.rem(tb + offset(i), n_tb)
        copy(to_ta * n_tb + to_tb, me, (to_ta, to_tb)).start()

    def send_step(i, _):
        for a in range(n_ta):
            send(i, a)
        return 0

    lax.fori_loop(0, n_tb - 1, send_step, 0)
    for a in range(1, n_ta):
        send(n_tb - 1, a)

    cls = regroup(me, lambda shift, block: turned_cls[shift, pl.ds(block, 1), :])
    for c in range(classes):
        basis_rows[c * pad : c * pad + lev, :] = basis_ref[c]
        basis_rows[c * pad + lev : (c + 1) * pad, :] = jnp.zeros((pad - lev, modes), jnp.bfloat16)
        mask[c] = jnp.broadcast_to((cls == c).astype(jnp.float32), (ROWS, col_dev)).astype(jnp.bfloat16)
    basis_t[...] = jnp.transpose(basis_rows[...])
    total_ref[...] = jnp.zeros_like(total_ref)

    def spread(x):
        x = x.reshape(pad // ROWS, ROWS, col_dev)
        return jnp.concatenate([(x * mask[c][None]).reshape(pad, col_dev) for c in range(classes)], axis=0)

    snaps = n

    def project(first, second):
        stacked = jnp.concatenate([spread(recv_buf[first]), spread(recv_buf[second])], axis=1)
        coef = jnp.dot(basis_t[...], stacked, preferred_element_type=jnp.float32)
        one, two = coef[:, :col_dev], coef[:, col_dev:]
        coef_ref[pl.ds(first, modes, stride=snaps), :] = one
        coef_ref[pl.ds(second, modes, stride=snaps), :] = two
        total_ref[...] += one + two

    def arrive(i, _):
        from_tb = lax.rem(tb + n_tb - offset(i), n_tb)
        for p in range(n_ta // 2):
            pair = [(2 * p + q) * n_tb + from_tb for q in range(2)]
            for src in pair:

                @pl.when(src != me)
                def _():
                    copy(src, src, (ta, tb)).wait_recv()

            project(*pair)
        return 0

    lax.fori_loop(0, n_tb, arrive, 0)

    def sent(k, _):
        dest = lax.rem(me + k, n)
        copy(dest, dest, (ta, tb)).wait_send()
        return 0

    lax.fori_loop(1, n, sent, 0)


def on_device(theta_cube, station_permutation_map, station_bathymetry_group, baroclinic_basis):
    instants, lev, cols = theta_cube.shape
    classes, _, modes = baroclinic_basis.shape
    n_ta = lax.axis_size("ta")
    n_tb = lax.axis_size("tb")
    n = n_ta * n_tb
    col_dev = cols // n
    pad = -(-lev // ROWS) * ROWS
    vmem = pl.BlockSpec(memory_space=pltpu.VMEM)
    coef, total = pl.pallas_call(
        functools.partial(exchange_kernel, n_ta, n_tb, col_dev),
        out_shape=(
            jax.ShapeDtypeStruct((modes * n, col_dev), jnp.float32),
            jax.ShapeDtypeStruct((modes, col_dev), jnp.float32),
        ),
        in_specs=[pl.BlockSpec(memory_space=pltpu.SMEM), vmem, vmem, vmem],
        out_specs=(vmem, vmem),
        scratch_shapes=[
            pltpu.VMEM((col_dev // TILE, n, lev, col_dev), jnp.bfloat16),
            pltpu.VMEM((col_dev // TILE, n, col_dev), jnp.int32),
            pltpu.VMEM((n, lev, col_dev), jnp.bfloat16),
            pltpu.VMEM((n, pad, col_dev), jnp.bfloat16),
            pltpu.VMEM((classes * pad, modes), jnp.bfloat16),
            pltpu.VMEM((modes, classes * pad), jnp.bfloat16),
            pltpu.VMEM((classes, ROWS, col_dev), jnp.bfloat16),
            pltpu.SemaphoreType.DMA((n,)),
            pltpu.SemaphoreType.DMA((n,)),
        ],
        compiler_params=pltpu.CompilerParams(
            collective_id=0, has_side_effects=True, vmem_limit_bytes=(16 if n <= 64 else 60) * 2**20
        ),
    )(
        station_permutation_map,
        theta_cube,
        station_bathymetry_group.reshape(cols // col_dev, col_dev),
        baroclinic_basis,
    )
    coef = coef.reshape(modes, n, col_dev)
    mean = total * (1.0 / n)
    return (coef - mean[:, None, :]).astype(jnp.bfloat16)


def solution(mesh):
    return jax.shard_map(
        on_device,
        mesh=mesh,
        in_specs=(P(("ta", "tb"), None, None), P(), P(), P()),
        out_specs=P(None, None, ("ta", "tb")),
        check_vma=False,
    )
```

```python
import functools

import jax
import jax.numpy as jnp
from jax import lax
from jax.experimental import pallas as pl
from jax.experimental.pallas import tpu as pltpu
from jax.sharding import PartitionSpec as P

TILE = 32
MESH = pl.DeviceIdType.MESH
ROWS = 16


def exchange_kernel(
    n_ta, n_tb, col_dev,
    perm_ref, theta_hbm, cls_hbm, basis_hbm,
    coef_ref, total_ref,
    theta_ref, cls_ref, basis_ref, basis_wide,
    turns, turned_cls, send_buf, recv_buf, basis_rows, basis_t, mask, load_sem, theta_sem, send_sem, recv_sem,
):
    n = n_ta * n_tb
    ta, tb = lax.axis_index("ta"), lax.axis_index("tb")
    me = ta * n_tb + tb
    _, lev, _ = theta_ref.shape
    _, classes, modes = basis_ref.shape
    pad = recv_buf.shape[1]
    per = col_dev // TILE

    def theta_load(block):
        lanes = pl.ds(pl.multiple_of(block * col_dev, col_dev), col_dev)
        return pltpu.make_async_copy(theta_hbm.at[0, :, lanes], theta_ref.at[block], theta_sem.at[block])

    def start_load(block, _):
        theta_load(block).start()
        return 0

    def wait_load(block, _):
        theta_load(block).wait()
        return 0

    cls_load = pltpu.make_async_copy(cls_hbm, cls_ref, load_sem.at[0])
    basis_load = pltpu.make_async_copy(basis_hbm, basis_ref, load_sem.at[1])
    lax.fori_loop(0, n, start_load, 0)
    cls_load.start()
    basis_load.start()

    barrier = pltpu.get_barrier_semaphore()

    def greet(k, _):
        other = lax.rem(me + k, n)
        pl.semaphore_signal(
            barrier, inc=1, device_id=(lax.div(other, n_tb), lax.rem(other, n_tb)), device_id_type=MESH
        )
        return 0

    lax.fori_loop(1, n, greet, 0)


    row = lax.broadcasted_iota(jnp.int32, (col_dev, col_dev), 0)
    lane = lax.broadcasted_iota(jnp.int32, (col_dev, col_dev), 1)
    for s in range(per):
        landed = lax.rem(row + s * TILE, col_dev) == lane
        for k in range(per):
            turns[k, s] = jnp.where(landed & (lane // TILE == k), 1.0, 0.0).astype(jnp.bfloat16)

    def group_place(dest, k):
        g = perm_ref[dest * per + k]
        return lax.div(g, per), lax.rem(k + per - lax.rem(g, per), per)

    def regroup(dest):
        pieces, moves = [], []
        for k in range(per):
            block, shift = group_place(dest, k)
            pieces.append(theta_ref[block])
            moves.append(turns[k, shift])
        return jnp.dot(
            jnp.concatenate(pieces, axis=1), jnp.concatenate(moves, axis=0), preferred_element_type=jnp.float32
        )

    recv_buf[:, lev:, :] = jnp.zeros((n, pad - lev, col_dev), jnp.bfloat16)
    lax.fori_loop(0, n, wait_load, 0)

    def prepare(dest):
        send_buf[dest] = regroup(dest).astype(jnp.bfloat16)

    pl.semaphore_wait(barrier, n - 1)

    def flip(place, by):
        out, bit = 0, 1
        while bit < max(n_ta, n_tb):
            out = out + bit * lax.rem(lax.div(place, bit) + lax.div(by, bit), 2)
            bit *= 2
        return out

    def offset(i):
        return (1 - lax.rem(i, 2)) * (n_tb // 2) + (n_tb // 2 - 1 - lax.div(i, 2))

    def copy(src, dst, device):
        return pltpu.make_async_remote_copy(
            src_ref=send_buf.at[src],
            dst_ref=recv_buf.at[dst, pl.ds(0, lev), :],
            send_sem=send_sem.at[src],
            recv_sem=recv_sem.at[dst],
            device_id=device,
            device_id_type=MESH,
        )

    def target(i, a):
        return flip(ta, a), flip(tb, offset(i))

    def prepare_step(i):
        for a in range(n_ta):
            to_ta, to_tb = target(i, a)
            prepare(to_ta * n_tb + to_tb)

    def send_step(i, first):
        for a in range(first, n_ta):
            to_ta, to_tb = target(i, a)
            copy(to_ta * n_tb + to_tb, me, (to_ta, to_tb)).start()

    prepare_step(0)

    def step(i, _):
        prepare_step(i + 1)
        send_step(i, 0)
        return 0

    lax.fori_loop(0, n_tb - 1, step, 0)
    recv_buf[me, :lev, :] = send_buf[me]
    send_step(n_tb - 1, 1)

    cls_load.wait()
    basis_load.wait()
    basis_wide[...] = basis_ref[...].reshape(lev * classes, modes).astype(jnp.float32)
    for k in range(per):
        turned_cls[k] = pltpu.roll(cls_ref[...], k * TILE, 1) if k else cls_ref[...]
    lane_group = lax.broadcasted_iota(jnp.int32, (1, col_dev), 1) // TILE
    cls = None
    for k in range(per):
        block, shift = group_place(me, k)
        piece = turned_cls[shift, pl.ds(block, 1), :]
        cls = piece if cls is None else jnp.where(lane_group == k, piece, cls)
    for c in range(classes):
        basis_rows[c * pad : c * pad + lev, :] = basis_wide[pl.ds(c, lev, stride=classes), :].astype(jnp.bfloat16)
        basis_rows[c * pad + lev : (c + 1) * pad, :] = jnp.zeros((pad - lev, modes), jnp.bfloat16)
        mask[c] = jnp.broadcast_to((cls == c).astype(jnp.float32), (ROWS, col_dev)).astype(jnp.bfloat16)
    basis_t[...] = jnp.transpose(basis_rows[...])
    total_ref[...] = jnp.zeros_like(total_ref)

    def spread(x):
        x = x.reshape(pad // ROWS, ROWS, col_dev)
        return jnp.concatenate([(x * mask[c][None]).reshape(pad, col_dev) for c in range(classes)], axis=0)

    snaps = n

    def project(first, second):
        stacked = jnp.concatenate([spread(recv_buf[first]), spread(recv_buf[second])], axis=1)
        coef = jnp.dot(basis_t[...], stacked, preferred_element_type=jnp.float32)
        one, two = coef[:, :col_dev], coef[:, col_dev:]
        coef_ref[pl.ds(first, modes, stride=snaps), :] = one
        coef_ref[pl.ds(second, modes, stride=snaps), :] = two
        total_ref[...] += one + two

    def arrive(i, _):
        from_tb = flip(tb, offset(i))
        for p in range(n_ta // 2):
            pair = [(2 * p + q) * n_tb + from_tb for q in range(2)]
            for src in pair:

                @pl.when(src != me)
                def _():
                    copy(src, src, (ta, tb)).wait_recv()

            project(*pair)
        return 0

    lax.fori_loop(0, n_tb, arrive, 0)

    def sent(k, _):
        dest = lax.rem(me + k, n)
        copy(dest, dest, (ta, tb)).wait_send()
        return 0

    lax.fori_loop(1, n, sent, 0)


def on_device(theta_cube, station_permutation_map, station_bathymetry_group, baroclinic_basis):
    instants, lev, cols = theta_cube.shape
    classes, _, modes = baroclinic_basis.shape
    n_ta = lax.axis_size("ta")
    n_tb = lax.axis_size("tb")
    n = n_ta * n_tb
    col_dev = cols // n
    pad = -(-lev // ROWS) * ROWS
    coef_bytes = 5 * (modes + 6) * (n + 1) * col_dev
    coef, total = pl.pallas_call(
        functools.partial(exchange_kernel, n_ta, n_tb, col_dev),
        out_shape=(
            pltpu.VMEM((modes * n, col_dev), jnp.float32),
            pltpu.VMEM((modes, col_dev), jnp.float32),
        ),
        in_specs=[pl.BlockSpec(memory_space=pltpu.SMEM)] + [pl.BlockSpec(memory_space=pltpu.HBM)] * 3,
        out_specs=(pl.BlockSpec(memory_space=pltpu.VMEM),) * 2,
        scratch_shapes=[
            pltpu.VMEM((n, lev, col_dev), jnp.bfloat16),
            pltpu.VMEM((cols // col_dev, col_dev), jnp.int32),
            pltpu.VMEM((lev, classes, modes), jnp.bfloat16),
            pltpu.VMEM((lev * classes, modes), jnp.float32),
            pltpu.VMEM((col_dev // TILE, col_dev // TILE, col_dev, col_dev), jnp.bfloat16),
            pltpu.VMEM((col_dev // TILE, cols // col_dev, col_dev), jnp.int32),
            pltpu.VMEM((n, lev, col_dev), jnp.bfloat16),
            pltpu.VMEM((n, pad, col_dev), jnp.bfloat16),
            pltpu.VMEM((classes * pad, modes), jnp.bfloat16),
            pltpu.VMEM((modes, classes * pad), jnp.bfloat16),
            pltpu.VMEM((classes, ROWS, col_dev), jnp.bfloat16),
            pltpu.SemaphoreType.DMA((2,)),
            pltpu.SemaphoreType.DMA((n,)),
            pltpu.SemaphoreType.DMA((n,)),
            pltpu.SemaphoreType.DMA((n,)),
        ],
        compiler_params=pltpu.CompilerParams(
            collective_id=0, has_side_effects=True, vmem_limit_bytes=67043328 - coef_bytes
        ),
    )(
        station_permutation_map,
        theta_cube,
        station_bathymetry_group.reshape(cols // col_dev, col_dev),
        jnp.transpose(baroclinic_basis, (1, 0, 2)),
    )
    coef = coef.reshape(modes, n, col_dev)
    mean = total * (1.0 / n)
    return (coef - mean[:, None, :]).astype(jnp.bfloat16)


def solution(mesh):
    return jax.shard_map(
        on_device,
        mesh=mesh,
        in_specs=(P(("ta", "tb"), None, None), P(), P(), P()),
        out_specs=P(None, None, ("ta", "tb")),
        check_vma=False,
    )
```
